32 devices in a mesh: blk: 8 (over z, y), grp: 4 (over x, core).
Axes of the slice: x: 2, y: 2, z: 4, core: 2. Of those that a mesh axis runs over, the one named last changes fastest.
Arguments:
- frames: bfloat16 [4, 2048, 1024], P('grp', 'blk'), may hold values from -16 to 16
- utt_lengths: int32 [4], replicated, may hold values from 1 to 4096, 8192 in all
- attn_gain: float32 [1024], replicated, may hold values from 0.25 to 1.75
- w_qkv: bfloat16 [1024, 3072], P(None, 'grp'), may hold values from -4 to 4
- w_out: bfloat16 [1024, 1024], replicated, may hold values from -0.375 to 0.375
- conv_gain: float32 [1024], replicated, may hold values from 0.25 to 1.75
- w_glu: bfloat16 [1024, 2048], replicated, may hold values from -0.1875 to 0.1875
- w_depth: float32 [31, 1024], replicated, may hold values from -1 to 1
- depth_gain: float32 [1024], replicated, may hold values from 0.25 to 1.75
- w_proj: bfloat16 [1024, 1024], replicated, may hold values from -0.1875 to 0.1875
Outputs:
- block_out: bfloat16 [4, 2048, 1024], P('grp', 'blk')
The draws below stay inside these ranges and needn't reach their ends.
Inputs may be any that keep to these rules, and one draw needn't show every extreme that they name: `utt_lengths`: they sum to 8192 and the longest is exactly 4096.
All inputs are finite; a program needn't handle non-finite values.
Results may differ from the reference program's by a relative error of at most 0.0095.
Values may be sent and summed in bfloat16 or wider, within the bound.
A program may use at most 192 MiB of HBM per device.

```python
import math
import jax
import jax.numpy as jnp
import numpy as np
from jax import lax

D = 1024
HEADS = 16
KERNEL = 31
WINDOW = 2048
GROUPS = 4
TOKENS = 8192
UTT_MOST = 4096
UTTERANCES = 4


def draw_frames(key, part):
    base_key = jax.random.fold_in(jax.random.fold_in(key, 11), 0)
    drawn = jax.random.normal(base_key, (GROUPS, WINDOW, D), jnp.float32)
    return jnp.clip(drawn, -16.0, 16.0).astype(jnp.bfloat16)


def draw_w_qkv(key, part):
    drawn = jax.random.normal(jax.random.fold_in(key, 23), (D, HEADS, 3, D // HEADS), jnp.float32) * (1.4 / math.sqrt(D))
    return jnp.clip(drawn.reshape(D, 3 * D), -4.0, 4.0).astype(jnp.bfloat16)


def length_profile(amount, total, most, slope):
    loads = [(1 << 20) // math.isqrt(grade ** slope) + 1 for grade in range(2, amount + 1)]
    surplus, counts = total - most - (amount - 1), [1] * (amount - 1)
    while surplus > 0:
        candidates = [i for i in range(amount - 1) if counts[i] < most]
        pool, remaining = sum([loads[i] for i in candidates]), surplus
        for i in candidates:
            addition = min(most - counts[i], max(1, remaining * loads[i] // pool), surplus)
            counts[i] = counts[i] + addition
            surplus = surplus - addition
    return np.array([most] + counts)


def ragged(own_key, count, total, reach, slope):
    if count == 2:
        one = jax.random.randint(own_key, (), max(1, total - reach), min(reach, total - 1) + 1)
        return jnp.stack([one, total - one])
    sizes = jnp.asarray(length_profile(count, total, reach, slope), jnp.int32)
    pairs = (count - 1) // 2
    donor, taker = sizes[1:1 + 2 * pairs:2], sizes[2:2 + 2 * pairs:2]
    slack = jnp.minimum(donor - 1, reach - taker)
    moved = jax.random.randint(jax.random.fold_in(own_key, 1), (pairs,), 0, 1 << 20) % (slack + 1)
    sizes = sizes.at[1:1 + 2 * pairs:2].set(donor - moved).at[2:2 + 2 * pairs:2].set(taker + moved)
    return sizes[jax.random.permutation(jax.random.fold_in(own_key, 2), count)]


def centred(stream_key, shape, scale, limit, held_as=jnp.bfloat16):
    values = scale * jax.random.normal(stream_key, shape, jnp.float32)
    return jnp.clip(values, min=-limit, max=limit).astype(held_as)


def setup_inputs(seed: int = 0) -> dict:
    splits = jax.random.split(jax.random.key(seed), 11)
    return {
        "frames": draw_frames(jax.random.fold_in(splits[10], 71), 0),
        "utt_lengths": ragged(splits[1], UTTERANCES, TOKENS, UTT_MOST, 2).astype(jnp.int32),
        "attn_gain": jnp.clip(1.0 + 0.15 * jax.random.normal(splits[2], (D,), jnp.float32), 0.25, 1.75),
        "w_qkv": draw_w_qkv(jax.random.fold_in(splits[10], 71), 0),
        "w_out": centred(splits[4], (D, D), (D // 4) ** -0.5, 0.375),
        "conv_gain": jnp.clip(1.0 + 0.15 * jax.random.normal(splits[5], (D,), jnp.float32), 0.25, 1.75),
        "w_glu": centred(splits[6], (D, 2 * D), D ** -0.5, 0.1875),
        "w_depth": centred(splits[7], (KERNEL, D), KERNEL ** -0.5, 1.0, jnp.float32),
        "depth_gain": jnp.clip(1.0 + 0.15 * jax.random.normal(splits[8], (D,), jnp.float32), 0.25, 1.75),
        "w_proj": centred(splits[9], (D, D), D ** -0.5, 0.1875),
    }


epsilon = 1e-05
big_negative = -1e+30

def normalize(values, row_gain):
    center = values - lax.optimization_barrier(jnp.mean(values, axis=-1, keepdims=True))
    spread = lax.optimization_barrier(jnp.mean(center * center, axis=-1, keepdims=True))
    return center * lax.rsqrt(spread + epsilon) * row_gain

def segment_of(utt_lengths, positions):
    starts = jnp.cumsum(utt_lengths) - utt_lengths
    started = (starts[None, :] <= positions[:, None]).astype(jnp.int32)
    return lax.optimization_barrier(jnp.sum(started, axis=1)) - 1

def one_head(head_qkv, seg_row, score_scale):
    scores = jnp.dot(head_qkv[0], head_qkv[1].T, preferred_element_type=jnp.float32) * score_scale
    allowed = seg_row[:, None] == seg_row[None, :]
    row_max = lax.optimization_barrier(jnp.max(jnp.where(allowed, scores, big_negative), axis=1, keepdims=True))
    weights = jnp.where(allowed, jnp.exp(scores - row_max), 0.0)
    row_total = lax.optimization_barrier(jnp.sum(weights, axis=1, keepdims=True))
    mixed_values = jnp.dot(weights.astype(jnp.bfloat16), head_qkv[2], preferred_element_type=jnp.float32)
    return mixed_values / row_total

def reference(frames, utt_lengths, attn_gain, w_qkv, w_out, conv_gain, w_glu, w_depth, depth_gain, w_proj):
    head_width = D // HEADS
    kernel_half = (KERNEL - 1) // 2
    score_scale = head_width ** (-0.5)
    flat_frames = frames.reshape(TOKENS, D)
    flat_float = flat_frames.astype(jnp.float32)
    frame_seg = segment_of(utt_lengths, jnp.arange(TOKENS, dtype=jnp.int32))
    normed = normalize(flat_float, attn_gain).astype(jnp.bfloat16)
    qkv_rows = jnp.dot(normed, w_qkv, preferred_element_type=jnp.float32).astype(jnp.bfloat16)
    arranged = jnp.transpose(qkv_rows.reshape(GROUPS, WINDOW, HEADS, 3, head_width), (0, 2, 3, 1, 4))
    group_seg = frame_seg.reshape(GROUPS, WINDOW)

    def one_group(operands):
        group_qkv, seg_row = operands
        return lax.map(lambda head_qkv: one_head(head_qkv, seg_row, score_scale), group_qkv)
    heads_out = lax.map(one_group, (arranged, group_seg))
    attended = jnp.transpose(heads_out, (0, 2, 1, 3)).reshape(TOKENS, D).astype(jnp.bfloat16)
    residual = (flat_float + jnp.dot(attended, w_out, preferred_element_type=jnp.float32)).astype(jnp.bfloat16)
    residual = lax.optimization_barrier(residual)
    conv_in = normalize(residual.astype(jnp.float32), conv_gain).astype(jnp.bfloat16)
    projected = jnp.dot(conv_in, w_glu, preferred_element_type=jnp.float32)
    gated = (projected[:, :D] * jax.nn.sigmoid(projected[:, D:])).astype(jnp.bfloat16)
    gated = lax.optimization_barrier(gated)
    padded = jnp.pad(gated.astype(jnp.float32), ((kernel_half, kernel_half), (0, 0)))
    pad_seg = segment_of(utt_lengths, jnp.arange(-kernel_half, TOKENS + kernel_half, dtype=jnp.int32))
    mixed_conv = jnp.zeros((TOKENS, D), jnp.float32)
    for offset in range(KERNEL):
        same_seg = (pad_seg[offset:offset + TOKENS] == frame_seg)[:, None]
        mixed_conv = mixed_conv + jnp.where(same_seg, padded[offset:offset + TOKENS] * w_depth[offset], 0.0)
    normed_conv = normalize(mixed_conv, depth_gain)
    activated = (normed_conv * jax.nn.sigmoid(normed_conv)).astype(jnp.bfloat16)
    result = (residual.astype(jnp.float32) + jnp.dot(activated, w_proj, preferred_element_type=jnp.float32)).astype(jnp.bfloat16)
    return result.reshape(GROUPS, WINDOW, D)
```

```python
import functools
import math

import jax
import jax.numpy as jnp
from jax import lax
from jax.experimental import pallas as pl
from jax.experimental.pallas import tpu as pltpu
from jax.sharding import PartitionSpec as P

HEADS = 16

epsilon = 1e-05
big_negative = -1e30
MESH = pl.DeviceIdType.MESH
VMEM_LIMIT = 56 * 1024 * 1024


def normalize(values, row_gain):
    center = values - jnp.mean(values, axis=-1, keepdims=True)
    spread = jnp.mean(center * center, axis=-1, keepdims=True)
    return center * lax.rsqrt(spread + epsilon) * row_gain


def seg_at(starts_ref, positions):
    seg = jnp.full(positions.shape, -1, jnp.int32)
    for c in range(starts_ref.shape[0]):
        seg = seg + jnp.where(positions >= starts_ref[c], 1, 0)
    return seg


def remote(src, dst, send, recv, blk, grp):
    return pltpu.make_async_remote_copy(
        src_ref=src, dst_ref=dst, send_sem=send, recv_sem=recv,
        device_id=(blk, grp), device_id_type=MESH,
    )


def project_kernel(
    blocks, groups, head_width, starts_ref, frames_ref, gain_ref, w_ref,
    q_ref, k_ref, v_ref,
    norm, held, weights, w_sem, d_sem, y_sem, p_sem, r_sem,
):
    b, g = lax.axis_index("blk"), lax.axis_index("grp")
    np_ = blocks // groups
    rows, width = frames_ref.shape
    columns = weights.shape[1]
    heads = columns // (3 * head_width)
    core, share, mine = g % 2, b % np_, b // np_
    partner = g + 1 - 2 * core
    if np_ == 1:
        w_src = w_ref
    else:
        w_src = w_ref.at[:, pl.ds(pl.multiple_of(share * columns, 128), columns)]
    w_copy = pltpu.make_async_copy(w_src, weights, w_sem)
    w_copy.start()
    norm[...] = normalize(frames_ref[...].astype(jnp.float32), gain_ref[...]).astype(jnp.bfloat16)
    side = (b // np_) % 2
    target = g * np_ + share

    def direct(k):
        return remote(norm, held.at[b], d_sem.at[k], r_sem.at[b], target, 2 * k + side)

    def is_self(k):
        return jnp.logical_and(target == b, 2 * k + side == g)

    for k in range(groups // 2):
        @pl.when(jnp.logical_not(is_self(k)))
        def _():
            direct(k).start()

    @pl.when(jnp.logical_and(target == b, side == core))
    def _():
        held[b] = norm[...]

    w_copy.wait()
    lane = lax.broadcasted_iota(jnp.int32, (rows, 128), 1)
    row = lax.broadcasted_iota(jnp.int32, (rows, 128), 0)
    scale = head_width ** (-0.5) * math.log2(math.e)

    def padded(part):
        return jnp.concatenate([part, jnp.zeros((rows, 128 - head_width), jnp.float32)], axis=1)

    def project(s):
        out = jnp.dot(held[s], weights[...], preferred_element_type=jnp.float32)
        seg = seg_at(starts_ref, (mine * blocks + s) * rows + row)
        same = lane - head_width == seg
        at = pl.ds(pl.multiple_of(s * rows, rows), rows)
        for h in range(heads):
            o = 3 * head_width * h
            q = padded(out[:, o:o + head_width] * scale)
            k = padded(out[:, o + head_width:o + 2 * head_width])
            v = padded(out[:, o + 2 * head_width:o + 3 * head_width])
            q = jnp.where(lane < head_width, q, jnp.where(same, big_negative, 0.0))
            k = jnp.where(lane < head_width, k, jnp.where(same, 0.0, 1.0))
            v = jnp.where(lane < head_width, v, jnp.where(lane == head_width, 1.0, 0.0))
            q_ref[h, at, :] = q.astype(jnp.bfloat16)
            k_ref[h, at, :] = k.astype(jnp.bfloat16)
            v_ref[h, at, :] = v.astype(jnp.bfloat16)

    def pair(s):
        return remote(held.at[s], held.at[s], p_sem.at[s], r_sem.at[s], b, partner)

    def across(s, i):
        other = mine * np_ + (share + i) % np_
        return remote(held.at[s], held.at[s], y_sem.at[s, i], r_sem.at[s], other, g)

    def first(j, carry):
        z = 2 * j + core
        s = z * np_ + share

        @pl.when(jnp.logical_not(jnp.logical_and(s == b, mine == g)))
        def _():
            pair(s).wait_recv()

        for i in range(1, np_):
            across(s, i).start()
        pair(s).start()
        project(s)
        for i in range(1, np_):
            t = z * np_ + (share + i) % np_
            pair(t).wait_recv()
            pair(t).start()
            project(t)
        return carry

    lax.fori_loop(0, groups // 2, first, 0)

    def second(j, carry):
        z = 2 * (j // np_) + 1 - core
        s = z * np_ + (share + j) % np_
        pair(s).wait_recv()
        project(s)
        return carry

    lax.fori_loop(0, blocks // 2, second, 0)

    for k in range(groups // 2):
        @pl.when(jnp.logical_not(is_self(k)))
        def _():
            direct(k).wait_send()

    def drain(j, carry):
        z = 2 * j + core
        for i in range(1, np_):
            across(z * np_ + share, i).wait_send()
        for i in range(np_):
            pair(z * np_ + i).wait_send()
        return carry

    lax.fori_loop(0, groups // 2, drain, 0)


def attend_kernel(head_width, q_ref, k_ref, v_ref, o_ref):
    outs = []
    for h in range(q_ref.shape[0]):
        scores = lax.dot_general(
            q_ref[h], k_ref[h], (((1,), (1,)), ((), ())), preferred_element_type=jnp.float32
        )
        top = jnp.max(scores, axis=1, keepdims=True)
        weights = jnp.exp2(scores - top).astype(jnp.bfloat16)
        mixed = jnp.dot(weights, v_ref[h], preferred_element_type=jnp.float32)
        outs.append(mixed[:, :head_width] / mixed[:, head_width:head_width + 1])
    o_ref[...] = jnp.concatenate(outs, axis=1).astype(o_ref.dtype)


def projected_and_attended(frames, starts, attn_gain, w_qkv, blocks, groups, head_width):
    rows, width = frames.shape
    np_ = blocks // groups
    columns = w_qkv.shape[1] // np_
    heads = columns // (3 * head_width)
    window = rows * blocks
    vm = pl.BlockSpec(memory_space=pltpu.VMEM)
    wide = jax.ShapeDtypeStruct((heads, window, 128), jnp.bfloat16)
    q, k, v = pl.pallas_call(
        functools.partial(project_kernel, blocks, groups, head_width),
        out_shape=[wide] * 3,
        in_specs=[pl.BlockSpec(memory_space=pltpu.SMEM), vm, vm, pl.BlockSpec(memory_space=pl.ANY)],
        out_specs=[vm] * 3,
        scratch_shapes=[
            pltpu.VMEM((rows, width), jnp.bfloat16),
            pltpu.VMEM((blocks, rows, width), jnp.bfloat16),
            pltpu.VMEM((width, columns), jnp.bfloat16),
            pltpu.SemaphoreType.DMA(()),
            pltpu.SemaphoreType.DMA((groups // 2,)),
            pltpu.SemaphoreType.DMA((blocks, np_)),
            pltpu.SemaphoreType.DMA((blocks,)),
            pltpu.SemaphoreType.DMA((blocks,)),
        ],
        compiler_params=pltpu.CompilerParams(has_side_effects=True, vmem_limit_bytes=VMEM_LIMIT),
        name="project",
    )(starts, frames, attn_gain[None], w_qkv)
    block = min(256, window)
    return pl.pallas_call(
        functools.partial(attend_kernel, head_width),
        grid=(window // block,),
        out_shape=jax.ShapeDtypeStruct((window, heads * head_width), jnp.bfloat16),
        in_specs=[
            pl.BlockSpec((heads, block, 128), lambda i: (0, i, 0)),
            pl.BlockSpec((heads, window, 128), lambda i: (0, 0, 0), pipeline_mode=pl.Buffered(1)),
            pl.BlockSpec((heads, window, 128), lambda i: (0, 0, 0), pipeline_mode=pl.Buffered(1)),
        ],
        out_specs=pl.BlockSpec((block, heads * head_width), lambda i: (i, 0)),
        compiler_params=pltpu.CompilerParams(vmem_limit_bytes=VMEM_LIMIT),
        name="attend",
    )(q, k, v)


def return_kernel(blocks, groups, o_ref, a_ref, s_sem, r_sem, l_sem):
    b, g = lax.axis_index("blk"), lax.axis_index("grp")
    np_ = blocks // groups
    rows = a_ref.shape[1]
    mine, unit = b // np_, g * np_ + b % np_

    def part(s):
        return o_ref.at[pl.ds(pl.multiple_of(s * rows, rows), rows)]

    def send(s):
        return remote(part(s), a_ref.at[unit], s_sem.at[s], r_sem.at[unit], s, mine)

    home = mine == g
    local = pltpu.make_async_copy(part(b), a_ref.at[unit], l_sem)

    @pl.when(home)
    def _():
        local.start()

    for i in range(blocks):
        s = (b + i) % blocks

        @pl.when(jnp.logical_not(jnp.logical_and(home, s == b)))
        def _():
            send(s).start()

    for i in range(blocks):
        @pl.when(jnp.logical_not(jnp.logical_and(home, unit == i)))
        def _():
            remote(a_ref.at[i], a_ref.at[i], s_sem.at[i], r_sem.at[i], b, g).wait_recv()

    for i in range(blocks):
        @pl.when(jnp.logical_not(jnp.logical_and(home, b == i)))
        def _():
            send(i).wait_send()

    @pl.when(home)
    def _():
        local.wait()


def padded_2(block, sides, width, periodic):
    for axis, dim in sides:
        count = lax.axis_size(axis)
        forward = [(i, i + 1) for i in range(count - 1)]
        if periodic:
            forward.append((count - 1, 0))
        backward = [(target, source) for source, target in forward]
        low = lax.ppermute(
            lax.slice_in_dim(block, block.shape[dim] - width, None, axis=dim), axis, forward
        )
        high = lax.ppermute(lax.slice_in_dim(block, 0, width, axis=dim), axis, backward)
        block = jnp.concatenate([low, block, high], axis=dim)
    return block


def segment_of(utt_lengths, positions):
    starts = jnp.cumsum(utt_lengths) - utt_lengths
    started = (starts[None, :] <= positions[:, None]).astype(jnp.int32)
    return jnp.sum(started, axis=1) - 1


def body(
    frames, utt_lengths, attn_gain, w_qkv, w_out, conv_gain, w_glu, w_depth, depth_gain, w_proj
):
    frame_rows = frames.shape[1]
    width = frames.shape[2]
    head_width = width // HEADS
    kernel_half = (w_depth.shape[0] - 1) // 2
    blocks, groups = lax.axis_size("blk"), lax.axis_size("grp")
    block_index = lax.axis_index("blk")
    group_index = lax.axis_index("grp")
    first_frame = (group_index * blocks + block_index) * frame_rows
    starts = jnp.cumsum(utt_lengths) - utt_lengths
    local_float = frames[0].astype(jnp.float32)
    mixed = projected_and_attended(frames[0], starts, attn_gain, w_qkv, blocks, groups, head_width)
    parts = pl.pallas_call(
        functools.partial(return_kernel, blocks, groups),
        out_shape=jax.ShapeDtypeStruct((blocks, frame_rows, mixed.shape[1]), jnp.bfloat16),
        in_specs=[pl.BlockSpec(memory_space=pltpu.VMEM)],
        out_specs=pl.BlockSpec(memory_space=pltpu.VMEM),
        scratch_shapes=[
            pltpu.SemaphoreType.DMA((blocks,)),
            pltpu.SemaphoreType.DMA((blocks,)),
            pltpu.SemaphoreType.DMA(()),
        ],
        compiler_params=pltpu.CompilerParams(has_side_effects=True),
        name="give_back",
    )(mixed)
    attended = jnp.transpose(parts, (1, 0, 2)).reshape(frame_rows, width)
    residual = (local_float + jnp.dot(attended, w_out, preferred_element_type=jnp.float32)).astype(
        jnp.bfloat16
    )
    residual = lax.optimization_barrier(residual)
    conv_in = normalize(residual.astype(jnp.float32), conv_gain).astype(jnp.bfloat16)
    projected = jnp.dot(conv_in, w_glu, preferred_element_type=jnp.float32)
    gated = (projected[:, :width] * jax.nn.sigmoid(projected[:, width:])).astype(jnp.bfloat16)
    gated = lax.optimization_barrier(gated)
    padded = padded_2(gated, (("blk", 0),), kernel_half, True)
    left_rim = padded[:kernel_half]
    right_rim = padded[frame_rows + kernel_half :]
    outer_rims = padded_2(jnp.stack([right_rim, left_rim]), (("grp", 0),), 1, False)
    left_edge = jnp.where(block_index == 0, outer_rims[0], left_rim)
    right_edge = jnp.where(block_index == blocks - 1, outer_rims[3], right_rim)
    extended = jnp.concatenate([left_edge, gated, right_edge], axis=0).astype(jnp.float32)
    local_seg = segment_of(utt_lengths, first_frame + jnp.arange(frame_rows, dtype=jnp.int32))
    extended_seg = segment_of(
        utt_lengths,
        first_frame - kernel_half + jnp.arange(frame_rows + 2 * kernel_half, dtype=jnp.int32),
    )
    mixed_conv = jnp.zeros((frame_rows, width), jnp.float32)
    for offset in range(2 * kernel_half + 1):
        same_seg = (extended_seg[offset : offset + frame_rows] == local_seg)[:, None]
        mixed_conv = mixed_conv + jnp.where(
            same_seg, extended[offset : offset + frame_rows] * w_depth[offset], 0.0
        )
    normed_conv = normalize(mixed_conv, depth_gain)
    activated = (normed_conv * jax.nn.sigmoid(normed_conv)).astype(jnp.bfloat16)
    result = (
        residual.astype(jnp.float32)
        + jnp.dot(activated, w_proj, preferred_element_type=jnp.float32)
    ).astype(jnp.bfloat16)
    return result[None]


def solution(mesh):
    in_specs = (P("grp", "blk", None), P(), P(), P(None, "grp"), P(), P(), P(), P(), P(), P())
    out_specs = P("grp", "blk", None)
    return jax.shard_map(body, mesh=mesh, in_specs=in_specs, out_specs=out_specs, check_vma=False)
```

```python
import functools
import math

import jax
import jax.numpy as jnp
from jax import lax
from jax.experimental import pallas as pl
from jax.experimental.pallas import tpu as pltpu
from jax.sharding import PartitionSpec as P

HEADS = 16

epsilon = 1e-05
big_negative = -1e30
MESH = pl.DeviceIdType.MESH
VMEM_LIMIT = 56 * 1024 * 1024


def normalize(values, row_gain):
    center = values - jnp.mean(values, axis=-1, keepdims=True)
    spread = jnp.mean(center * center, axis=-1, keepdims=True)
    return center * lax.rsqrt(spread + epsilon) * row_gain


def seg_at(starts_ref, positions):
    seg = jnp.full(positions.shape, -1, jnp.int32)
    for c in range(starts_ref.shape[0]):
        seg = seg + jnp.where(positions >= starts_ref[c], 1, 0)
    return seg


def remote(src, dst, send, recv, blk, grp):
    return pltpu.make_async_remote_copy(
        src_ref=src, dst_ref=dst, send_sem=send, recv_sem=recv,
        device_id=(blk, grp), device_id_type=MESH,
    )


def place_of(window, groups):
    return (window % 2) * (groups // 2) + window // 2


def window_at(place, groups):
    return (place % (groups // 2)) * 2 + place // (groups // 2)


def project_kernel(
    blocks, groups, head_width, starts_ref, frames_ref, gain_ref, w_ref,
    q_ref, k_ref, v_ref,
    norm, held, weights, w_sem, d_sem, y_sem, p_sem, r_sem,
):
    b, g = lax.axis_index("blk"), lax.axis_index("grp")
    np_ = blocks // groups
    rows, width = frames_ref.shape
    columns = weights.shape[1]
    heads = columns // (3 * head_width)
    core, share, mine = g % 2, b % np_, window_at(b // np_, groups)
    partner = g + 1 - 2 * core
    if np_ == 1:
        w_src = w_ref
    else:
        w_src = w_ref.at[:, pl.ds(pl.multiple_of(share * columns, 128), columns)]
    w_copy = pltpu.make_async_copy(w_src, weights, w_sem)
    w_copy.start()
    norm[...] = normalize(frames_ref[...].astype(jnp.float32), gain_ref[...]).astype(jnp.bfloat16)
    side = (b // np_) % 2
    target = place_of(g, groups) * np_ + share

    def direct(k):
        return remote(norm, held.at[b], d_sem.at[k], r_sem.at[b], target, 2 * k + side)

    def is_self(k):
        return jnp.logical_and(target == b, 2 * k + side == g)

    for k in range(groups // 2):
        @pl.when(jnp.logical_not(is_self(k)))
        def _():
            direct(k).start()

    @pl.when(jnp.logical_and(target == b, side == core))
    def _():
        held[b] = norm[...]

    w_copy.wait()
    lane = lax.broadcasted_iota(jnp.int32, (rows, 128), 1)
    row = lax.broadcasted_iota(jnp.int32, (rows, 128), 0)
    scale = head_width ** (-0.5) * math.log2(math.e)

    def padded(part):
        return jnp.concatenate([part, jnp.zeros((rows, 128 - head_width), jnp.float32)], axis=1)

    def project(s):
        out = jnp.dot(held[s], weights[...], preferred_element_type=jnp.float32)
        seg = seg_at(starts_ref, (mine * blocks + s) * rows + row)
        same = lane - head_width == seg
        at = pl.ds(pl.multiple_of(s * rows, rows), rows)
        for h in range(heads):
            o = 3 * head_width * h
            q = padded(out[:, o:o + head_width] * scale)
            k = padded(out[:, o + head_width:o + 2 * head_width])
            v = padded(out[:, o + 2 * head_width:o + 3 * head_width])
            q = jnp.where(lane < head_width, q, jnp.where(same, big_negative, 0.0))
            k = jnp.where(lane < head_width, k, jnp.where(same, 0.0, 1.0))
            v = jnp.where(lane < head_width, v, jnp.where(lane == head_width, 1.0, 0.0))
            q_ref[h, at, :] = q.astype(jnp.bfloat16)
            k_ref[h, at, :] = k.astype(jnp.bfloat16)
            v_ref[h, at, :] = v.astype(jnp.bfloat16)

    def pair(s):
        return remote(held.at[s], held.at[s], p_sem.at[s], r_sem.at[s], b, partner)

    def across(s, i):
        other = b - share + (share + i) % np_
        return remote(held.at[s], held.at[s], y_sem.at[s, i], r_sem.at[s], other, g)

    def first(j, carry):
        z = 2 * j + core
        s = z * np_ + share

        @pl.when(jnp.logical_not(jnp.logical_and(s == b, mine == g)))
        def _():
            pair(s).wait_recv()

        for i in range(1, np_):
            across(s, i).start()
        pair(s).start()
        project(s)
        for i in range(1, np_):
            t = z * np_ + (share + i) % np_
            pair(t).wait_recv()
            pair(t).start()
            project(t)
        return carry

    lax.fori_loop(0, groups // 2, first, 0)

    def second(j, carry):
        z = 2 * (j // np_) + 1 - core
        s = z * np_ + (share + j) % np_
        pair(s).wait_recv()
        project(s)
        return carry

    lax.fori_loop(0, blocks // 2, second, 0)

    for k in range(groups // 2):
        @pl.when(jnp.logical_not(is_self(k)))
        def _():
            direct(k).wait_send()

    def drain(j, carry):
        z = 2 * j + core
        for i in range(1, np_):
            across(z * np_ + share, i).wait_send()
        for i in range(np_):
            pair(z * np_ + i).wait_send()
        return carry

    lax.fori_loop(0, groups // 2, drain, 0)


def attend_kernel(head_width, q_ref, k_ref, v_ref, o_ref):
    outs = []
    for h in range(q_ref.shape[0]):
        scores = lax.dot_general(
            q_ref[h], k_ref[h], (((1,), (1,)), ((), ())), preferred_element_type=jnp.float32
        )
        top = jnp.max(scores, axis=1, keepdims=True)
        weights = jnp.exp2(scores - top).astype(jnp.bfloat16)
        mixed = jnp.dot(weights, v_ref[h], preferred_element_type=jnp.float32)
        outs.append(mixed[:, :head_width] / mixed[:, head_width:head_width + 1])
    o_ref[...] = jnp.concatenate(outs, axis=1).astype(o_ref.dtype)


def projected_and_attended(frames, starts, attn_gain, w_qkv, blocks, groups, head_width):
    rows, width = frames.shape
    np_ = blocks // groups
    columns = w_qkv.shape[1] // np_
    heads = columns // (3 * head_width)
    window = rows * blocks
    vm = pl.BlockSpec(memory_space=pltpu.VMEM)
    wide = jax.ShapeDtypeStruct((heads, window, 128), jnp.bfloat16)
    q, k, v = pl.pallas_call(
        functools.partial(project_kernel, blocks, groups, head_width),
        out_shape=[wide] * 3,
        in_specs=[pl.BlockSpec(memory_space=pltpu.SMEM), vm, vm, pl.BlockSpec(memory_space=pl.ANY)],
        out_specs=[vm] * 3,
        scratch_shapes=[
            pltpu.VMEM((rows, width), jnp.bfloat16),
            pltpu.VMEM((blocks, rows, width), jnp.bfloat16),
            pltpu.VMEM((width, columns), jnp.bfloat16),
            pltpu.SemaphoreType.DMA(()),
            pltpu.SemaphoreType.DMA((groups // 2,)),
            pltpu.SemaphoreType.DMA((blocks, np_)),
            pltpu.SemaphoreType.DMA((blocks,)),
            pltpu.SemaphoreType.DMA((blocks,)),
        ],
        compiler_params=pltpu.CompilerParams(has_side_effects=True, vmem_limit_bytes=VMEM_LIMIT),
        name="project",
    )(starts, frames, attn_gain[None], w_qkv)
    block = min(256, window)
    return pl.pallas_call(
        functools.partial(attend_kernel, head_width),
        grid=(window // block,),
        out_shape=jax.ShapeDtypeStruct((window, heads * head_width), jnp.bfloat16),
        in_specs=[
            pl.BlockSpec((heads, block, 128), lambda i: (0, i, 0)),
            pl.BlockSpec((heads, window, 128), lambda i: (0, 0, 0), pipeline_mode=pl.Buffered(1)),
            pl.BlockSpec((heads, window, 128), lambda i: (0, 0, 0), pipeline_mode=pl.Buffered(1)),
        ],
        out_specs=pl.BlockSpec((block, heads * head_width), lambda i: (i, 0)),
        compiler_params=pltpu.CompilerParams(vmem_limit_bytes=VMEM_LIMIT),
        name="attend",
    )(q, k, v)


def finish_kernel(
    blocks, groups, starts_ref, o_ref, frames_ref, conv_gain_ref, depth_ref, depth_gain_ref,
    w_out_ref, w_glu_ref, w_proj_ref,
    out_ref,
    parts, w_out, w_glu, w_proj, masks, residual, edge, halo, extended, mixed,
    s_sem, r_sem, l_sem, w_sem, hs_sem, hr_sem,
):
    b, g = lax.axis_index("blk"), lax.axis_index("grp")
    np_ = blocks // groups
    rows, width = frames_ref.shape
    taps = depth_ref.shape[0]
    half = (taps - 1) // 2
    rim = halo.shape[1]
    mine, unit = window_at(b // np_, groups), g * np_ + b % np_
    home = mine == g
    position = g * blocks + b
    after = (position + 1) % (blocks * groups)
    before = (position + blocks * groups - 1) % (blocks * groups)

    def part(s):
        return o_ref.at[pl.ds(pl.multiple_of(s * rows, rows), rows)]

    def send(s):
        return remote(part(s), parts.at[unit], s_sem.at[s], r_sem.at[unit], s, mine)

    local = pltpu.make_async_copy(part(b), parts.at[unit], l_sem)

    @pl.when(home)
    def _():
        local.start()

    for i in range(blocks):
        s = (b + i) % blocks

        @pl.when(jnp.logical_not(jnp.logical_and(home, s == b)))
        def _():
            send(s).start()

    loads = [
        pltpu.make_async_copy(w_out_ref, w_out, w_sem.at[0]),
        pltpu.make_async_copy(w_glu_ref, w_glu, w_sem.at[1]),
        pltpu.make_async_copy(w_proj_ref, w_proj, w_sem.at[2]),
    ]
    for load in loads:
        load.start()

    row = position * rows + lax.broadcasted_iota(jnp.int32, (rows, 128), 0)
    low = jnp.zeros((rows, 128), jnp.int32)
    high = jnp.full((rows, 128), blocks * groups * rows, jnp.int32)
    for c in range(starts_ref.shape[0]):
        start = starts_ref[c]
        low = jnp.where(row >= start, jnp.maximum(low, start), low)
        high = jnp.where(row < start, jnp.minimum(high, start), high)
    for t in range(taps):
        at = row + (t - half)
        masks[t] = jnp.where(jnp.logical_and(at >= low, at < high), 1.0, 0.0)

    @pl.when(home)
    def _():
        local.wait()

    for i in range(blocks):
        @pl.when(jnp.logical_not(jnp.logical_and(home, unit == i)))
        def _():
            remote(parts.at[i], parts.at[i], s_sem.at[i], r_sem.at[i], b, g).wait_recv()

    attended = jnp.concatenate([parts[i] for i in range(blocks)], axis=1)
    loads[0].wait()
    total = frames_ref[...].astype(jnp.float32) + jnp.dot(
        attended, w_out[...], preferred_element_type=jnp.float32
    )
    residual[...] = total.astype(jnp.bfloat16)
    conv_in = normalize(residual[...].astype(jnp.float32), conv_gain_ref[...]).astype(jnp.bfloat16)
    loads[1].wait()
    step = 256
    for n in range(0, width, step):
        a = jnp.dot(conv_in, w_glu[:, n:n + step], preferred_element_type=jnp.float32)
        gate = jnp.dot(
            conv_in, w_glu[:, width + n:width + n + step], preferred_element_type=jnp.float32
        )
        gated = (a * jax.nn.sigmoid(gate)).astype(jnp.bfloat16)
        edge[0, :, n:n + step] = gated[:rim]
        edge[1, :, n:n + step] = gated[rows - rim:]
        extended[rim:rim + rows, n:n + step] = gated.astype(jnp.float32)

    to_next = remote(
        edge.at[1], halo.at[0], hs_sem.at[1], hr_sem.at[0], after % blocks, after // blocks
    )
    to_prev = remote(
        edge.at[0], halo.at[1], hs_sem.at[0], hr_sem.at[1], before % blocks, before // blocks
    )
    to_next.start()
    to_prev.start()

    strip = min(64, rows)

    def convolve(strips):
        def column(c, carry):
            cols = pl.ds(pl.multiple_of(c * 128, 128), 128)
            for r in strips:
                acc = jnp.zeros((strip, 128), jnp.float32)
                for t in range(taps):
                    e = rim + r + t - half
                    x = extended[e:e + strip, cols] * masks[t, r:r + strip, :]
                    acc = acc + x * depth_ref[t:t + 1, cols]
                mixed[r:r + strip, cols] = acc
            return carry

        lax.fori_loop(0, width // 128, column, 0)

    every = list(range(0, rows, strip))
    convolve(every[1:-1])
    to_next.wait_recv()
    to_prev.wait_recv()
    extended[:rim, :] = halo[0].astype(jnp.float32)
    extended[rim + rows:, :] = halo[1].astype(jnp.float32)
    convolve([every[0], every[-1]])
    normed = normalize(mixed[...], depth_gain_ref[...])
    activated = (normed * jax.nn.sigmoid(normed)).astype(jnp.bfloat16)
    loads[2].wait()
    out_ref[0] = (
        residual[...].astype(jnp.float32)
        + jnp.dot(activated, w_proj[...], preferred_element_type=jnp.float32)
    ).astype(out_ref.dtype)

    for i in range(blocks):
        @pl.when(jnp.logical_not(jnp.logical_and(home, b == i)))
        def _():
            send(i).wait_send()

    to_next.wait_send()
    to_prev.wait_send()


def body(
    frames, utt_lengths, attn_gain, w_qkv, w_out, conv_gain, w_glu, w_depth, depth_gain, w_proj
):
    rows, width = frames.shape[1:]
    blocks, groups = lax.axis_size("blk"), lax.axis_size("grp")
    starts = jnp.cumsum(utt_lengths) - utt_lengths
    mixed = projected_and_attended(
        frames[0], starts, attn_gain, w_qkv, blocks, groups, width // HEADS
    )
    taps = w_depth.shape[0]
    rim = -(-(taps // 2) // 16) * 16
    vm = pl.BlockSpec(memory_space=pltpu.VMEM)
    hbm = pl.BlockSpec(memory_space=pl.ANY)
    return pl.pallas_call(
        functools.partial(finish_kernel, blocks, groups),
        out_shape=jax.ShapeDtypeStruct((1, rows, width), jnp.bfloat16),
        in_specs=[pl.BlockSpec(memory_space=pltpu.SMEM)] + [vm] * 5 + [hbm] * 3,
        out_specs=vm,
        scratch_shapes=[
            pltpu.VMEM((blocks, rows, mixed.shape[1]), jnp.bfloat16),
            pltpu.VMEM(w_out.shape, jnp.bfloat16),
            pltpu.VMEM(w_glu.shape, jnp.bfloat16),
            pltpu.VMEM(w_proj.shape, jnp.bfloat16),
            pltpu.VMEM((taps, rows, 128), jnp.float32),
            pltpu.VMEM((rows, width), jnp.bfloat16),
            pltpu.VMEM((2, rim, width), jnp.bfloat16),
            pltpu.VMEM((2, rim, width), jnp.bfloat16),
            pltpu.VMEM((rows + 2 * rim, width), jnp.float32),
            pltpu.VMEM((rows, width), jnp.float32),
            pltpu.SemaphoreType.DMA((blocks,)),
            pltpu.SemaphoreType.DMA((blocks,)),
            pltpu.SemaphoreType.DMA(()),
            pltpu.SemaphoreType.DMA((3,)),
            pltpu.SemaphoreType.DMA((2,)),
            pltpu.SemaphoreType.DMA((2,)),
        ],
        compiler_params=pltpu.CompilerParams(has_side_effects=True, vmem_limit_bytes=VMEM_LIMIT),
        name="finish",
    )(starts, mixed, frames[0], conv_gain[None], w_depth, depth_gain[None], w_out, w_glu, w_proj)


def solution(mesh):
    in_specs = (P("grp", "blk", None), P(), P(), P(None, "grp"), P(), P(), P(), P(), P(), P())
    out_specs = P("grp", "blk", None)
    return jax.shard_map(body, mesh=mesh, in_specs=in_specs, out_specs=out_specs, check_vma=False)
```

```python
import functools
import math

import jax
import jax.numpy as jnp
from jax import lax
from jax.experimental import pallas as pl
from jax.experimental.pallas import tpu as pltpu
from jax.sharding import PartitionSpec as P

HEADS = 16

epsilon = 1e-05
big_negative = -1e30
MESH = pl.DeviceIdType.MESH
VMEM_LIMIT = 56 * 1024 * 1024


def normalize(values, row_gain):
    center = values - jnp.mean(values, axis=-1, keepdims=True)
    spread = jnp.mean(center * center, axis=-1, keepdims=True)
    return center * lax.rsqrt(spread + epsilon) * row_gain


def starts_of(lengths_ref):
    starts, total = [], jnp.int32(0)
    for c in range(lengths_ref.shape[0]):
        starts.append(total)
        total = total + lengths_ref[c]
    return starts


def seg_at(starts, positions):
    seg = jnp.full(positions.shape, -1, jnp.int32)
    for start in starts:
        seg = seg + jnp.where(positions >= start, 1, 0)
    return seg


def remote(src, dst, send, recv, blk, grp):
    return pltpu.make_async_remote_copy(
        src_ref=src, dst_ref=dst, send_sem=send, recv_sem=recv,
        device_id=(blk, grp), device_id_type=MESH,
    )


def place_of(window, groups):
    return (window % 2) * (groups // 2) + window // 2


def window_at(place, groups):
    return (place % (groups // 2)) * 2 + place // (groups // 2)


def project_kernel(
    blocks, groups, chunks, head_width, lengths_ref, frames_ref, gain_ref, w_ref,
    q_ref, k_ref, v_ref,
    norm, held, weights, w_sem, d_sem, x_sem, y_sem, p_sem, r_sem,
):
    b, g = lax.axis_index("blk"), lax.axis_index("grp")
    np_ = blocks // groups
    pairs = groups // 2
    rows, width = norm.shape[1:]
    columns = weights.shape[1]
    heads = columns // (3 * head_width)
    place, share, core, chip = b // np_, b % np_, g % 2, g // 2
    mine = window_at(place, groups)
    source_chip = mine // 2
    partner = g + 1 - 2 * core
    if np_ == 1:
        w_src = w_ref
    else:
        w_src = w_ref.at[:, pl.ds(pl.multiple_of(share * columns, 128), columns)]
    w_copy = pltpu.make_async_copy(w_src, weights, w_sem)
    w_copy.start()
    target = place_of(g, groups) * np_ + share
    target_core = place % 2
    self_kept = jnp.logical_and(target == b, target_core == core)

    def direct(c):
        u = b * chunks + c
        return remote(
            norm.at[c], held.at[u], d_sem.at[c], r_sem.at[u], target, 2 * chip + target_core
        )

    for c in range(chunks):
        part = frames_ref[c * rows:(c + 1) * rows, :].astype(jnp.float32)
        norm[c] = normalize(part, gain_ref[...]).astype(jnp.bfloat16)

        @pl.when(jnp.logical_not(self_kept))
        def _():
            direct(c).start()

        @pl.when(self_kept)
        def _():
            held[b * chunks + c] = norm[c]

    lane = lax.broadcasted_iota(jnp.int32, (rows, 128), 1)
    row = lax.broadcasted_iota(jnp.int32, (rows, 128), 0)
    scale = head_width ** (-0.5) * math.log2(math.e)
    starts = starts_of(lengths_ref)

    def padded(part):
        return jnp.concatenate([part, jnp.zeros((rows, 128 - head_width), jnp.float32)], axis=1)

    def project(u):
        out = jnp.dot(held[u], weights[...], preferred_element_type=jnp.float32)
        seg = seg_at(starts, mine * blocks * chunks * rows + u * rows + row)
        same = lane - head_width == seg
        at = pl.ds(pl.multiple_of(u * rows, rows), rows)
        for h in range(heads):
            o = 3 * head_width * h
            q = padded(out[:, o:o + head_width] * scale)
            k = padded(out[:, o + head_width:o + 2 * head_width])
            v = padded(out[:, o + 2 * head_width:o + 3 * head_width])
            q = jnp.where(lane < head_width, q, jnp.where(same, big_negative, 0.0))
            k = jnp.where(lane < head_width, k, jnp.where(same, 0.0, 1.0))
            v = jnp.where(lane < head_width, v, jnp.where(lane == head_width, 1.0, 0.0))
            q_ref[h, at, :] = q.astype(jnp.bfloat16)
            k_ref[h, at, :] = k.astype(jnp.bfloat16)
            v_ref[h, at, :] = v.astype(jnp.bfloat16)

    def pair(u):
        return remote(held.at[u], held.at[u], p_sem.at[u], r_sem.at[u], b, partner)

    def across(u, i):
        other = b - share + (share + i) % np_
        return remote(held.at[u], held.at[u], y_sem.at[u, i], r_sem.at[u], other, g)

    def over(u, k):
        return remote(held.at[u], held.at[u], x_sem.at[u, k], r_sem.at[u], b, 2 * k + core)

    def unit(j, i):
        n = j // chunks
        n = n + place // pairs * (pairs - 1 - 2 * n)
        return ((2 * n + core) * np_ + (share + i) % np_) * chunks + j % chunks

    count = pairs * chunks

    def take(j, carry):
        u = unit(j, 0)

        @pl.when(jnp.logical_not(jnp.logical_and(u // chunks == b, mine == g)))
        def _():
            pair(u).wait_recv()

        for k in range(pairs):
            @pl.when(jnp.logical_and(chip == source_chip, chip != k))
            def _():
                over(u, k).start()

        for i in range(1, np_):
            across(u, i).start()
        pair(u).start()
        return carry

    lax.fori_loop(0, count, take, 0)
    w_copy.wait()

    def own(j, carry):
        project(unit(j, 0))
        return carry

    lax.fori_loop(0, count, own, 0)

    def pass_on(j, carry):
        for i in range(1, np_):
            u = unit(j, i)
            pair(u).wait_recv()
            pair(u).start()
            project(u)
        return carry

    if np_ > 1:
        lax.fori_loop(0, count, pass_on, 0)

    def rest(j, carry):
        n = j // (np_ * chunks)
        n = n + place // pairs * (pairs - 1 - 2 * n)
        i = j // chunks % np_
        u = ((2 * n + 1 - core) * np_ + (share + i) % np_) * chunks + j % chunks
        pair(u).wait_recv()
        project(u)
        return carry

    lax.fori_loop(0, count * np_, rest, 0)

    for c in range(chunks):
        @pl.when(jnp.logical_not(self_kept))
        def _():
            direct(c).wait_send()

    def drain(j, carry):
        u = unit(j, 0)
        for k in range(pairs):
            @pl.when(jnp.logical_and(chip == source_chip, chip != k))
            def _():
                over(u, k).wait_send()

        for i in range(1, np_):
            across(u, i).wait_send()
        for i in range(np_):
            pair(unit(j, i)).wait_send()
        return carry

    lax.fori_loop(0, count, drain, 0)


def attend_kernel(head_width, q_ref, k_ref, v_ref, o_ref):
    outs = []
    for h in range(q_ref.shape[0]):
        scores = lax.dot_general(
            q_ref[h], k_ref[h], (((1,), (1,)), ((), ())), preferred_element_type=jnp.float32
        )
        top = jnp.max(scores, axis=1, keepdims=True)
        weights = jnp.exp2(scores - top).astype(jnp.bfloat16)
        mixed = jnp.dot(weights, v_ref[h], preferred_element_type=jnp.float32)
        outs.append(mixed[:, :head_width] / mixed[:, head_width:head_width + 1])
    o_ref[...] = jnp.concatenate(outs, axis=1).astype(o_ref.dtype)


def projected_and_attended(frames, lengths, attn_gain, w_qkv, blocks, groups, head_width):
    rows, width = frames.shape
    np_ = blocks // groups
    columns = w_qkv.shape[1] // np_
    heads = columns // (3 * head_width)
    window = rows * blocks
    chunks = 2 if rows % 32 == 0 else 1
    vm = pl.BlockSpec(memory_space=pltpu.VMEM)
    wide = jax.ShapeDtypeStruct((heads, window, 128), jnp.bfloat16)
    q, k, v = pl.pallas_call(
        functools.partial(project_kernel, blocks, groups, chunks, head_width),
        out_shape=[wide] * 3,
        in_specs=[pl.BlockSpec(memory_space=pltpu.SMEM), vm, vm, pl.BlockSpec(memory_space=pl.ANY)],
        out_specs=[vm] * 3,
        scratch_shapes=[
            pltpu.VMEM((chunks, rows // chunks, width), jnp.bfloat16),
            pltpu.VMEM((blocks * chunks, rows // chunks, width), jnp.bfloat16),
            pltpu.VMEM((width, columns), jnp.bfloat16),
            pltpu.SemaphoreType.DMA(()),
            pltpu.SemaphoreType.DMA((chunks,)),
            pltpu.SemaphoreType.DMA((blocks * chunks, groups // 2)),
            pltpu.SemaphoreType.DMA((blocks * chunks, np_)),
            pltpu.SemaphoreType.DMA((blocks * chunks,)),
            pltpu.SemaphoreType.DMA((blocks * chunks,)),
        ],
        compiler_params=pltpu.CompilerParams(has_side_effects=True, vmem_limit_bytes=VMEM_LIMIT),
        name="project",
    )(lengths, frames, attn_gain[None], w_qkv)
    block = min(256, window)
    return pl.pallas_call(
        functools.partial(attend_kernel, head_width),
        grid=(window // block,),
        out_shape=jax.ShapeDtypeStruct((window, heads * head_width), jnp.bfloat16),
        in_specs=[
            pl.BlockSpec((heads, block, 128), lambda i: (0, i, 0)),
            pl.BlockSpec((heads, window, 128), lambda i: (0, 0, 0), pipeline_mode=pl.Buffered(1)),
            pl.BlockSpec((heads, window, 128), lambda i: (0, 0, 0), pipeline_mode=pl.Buffered(1)),
        ],
        out_specs=pl.BlockSpec((block, heads * head_width), lambda i: (i, 0)),
        compiler_params=pltpu.CompilerParams(vmem_limit_bytes=VMEM_LIMIT),
        name="attend",
    )(q, k, v)


def finish_kernel(
    blocks, groups, lengths_ref, o_ref, frames_ref, conv_gain_ref, depth_ref, depth_gain_ref,
    w_out_ref, w_glu_ref, w_proj_ref,
    out_ref,
    parts, w_out, w_glu, w_proj, masks, residual, edge, halo, extended, mixed,
    s_sem, r_sem, l_sem, w_sem, hs_sem, hr_sem,
):
    b, g = lax.axis_index("blk"), lax.axis_index("grp")
    np_ = blocks // groups
    rows, width = frames_ref.shape
    taps = depth_ref.shape[0]
    half = (taps - 1) // 2
    rim = halo.shape[1]
    mine, unit = window_at(b // np_, groups), g * np_ + b % np_
    home = mine == g
    position = g * blocks + b
    after = (position + 1) % (blocks * groups)
    before = (position + blocks * groups - 1) % (blocks * groups)

    def part(s):
        return o_ref.at[pl.ds(pl.multiple_of(s * rows, rows), rows)]

    def send(s):
        return remote(part(s), parts.at[unit], s_sem.at[s], r_sem.at[unit], s, mine)

    local = pltpu.make_async_copy(part(b), parts.at[unit], l_sem)

    @pl.when(home)
    def _():
        local.start()

    for i in range(blocks):
        s = (b + i) % blocks

        @pl.when(jnp.logical_not(jnp.logical_and(home, s == b)))
        def _():
            send(s).start()

    loads = [
        pltpu.make_async_copy(w_out_ref, w_out, w_sem.at[0]),
        pltpu.make_async_copy(w_glu_ref, w_glu, w_sem.at[1]),
        pltpu.make_async_copy(w_proj_ref, w_proj, w_sem.at[2]),
    ]
    for load in loads:
        load.start()

    row = position * rows + lax.broadcasted_iota(jnp.int32, (rows, 128), 0)
    low = jnp.zeros((rows, 128), jnp.int32)
    high = jnp.full((rows, 128), blocks * groups * rows, jnp.int32)
    for start in starts_of(lengths_ref):
        low = jnp.where(row >= start, jnp.maximum(low, start), low)
        high = jnp.where(row < start, jnp.minimum(high, start), high)
    for t in range(taps):
        at = row + (t - half)
        masks[t] = jnp.where(jnp.logical_and(at >= low, at < high), 1.0, 0.0)

    @pl.when(home)
    def _():
        local.wait()

    for i in range(blocks):
        @pl.when(jnp.logical_not(jnp.logical_and(home, unit == i)))
        def _():
            remote(parts.at[i], parts.at[i], s_sem.at[i], r_sem.at[i], b, g).wait_recv()

    attended = jnp.concatenate([parts[i] for i in range(blocks)], axis=1)
    loads[0].wait()
    total = frames_ref[...].astype(jnp.float32) + jnp.dot(
        attended, w_out[...], preferred_element_type=jnp.float32
    )
    residual[...] = total.astype(jnp.bfloat16)
    conv_in = normalize(residual[...].astype(jnp.float32), conv_gain_ref[...]).astype(jnp.bfloat16)
    loads[1].wait()
    step = 256
    for n in range(0, width, step):
        a = jnp.dot(conv_in, w_glu[:, n:n + step], preferred_element_type=jnp.float32)
        gate = jnp.dot(
            conv_in, w_glu[:, width + n:width + n + step], preferred_element_type=jnp.float32
        )
        gated = (a * jax.nn.sigmoid(gate)).astype(jnp.bfloat16)
        edge[0, :, n:n + step] = gated[:rim]
        edge[1, :, n:n + step] = gated[rows - rim:]
        extended[rim:rim + rows, n:n + step] = gated.astype(jnp.float32)

    to_next = remote(
        edge.at[1], halo.at[0], hs_sem.at[1], hr_sem.at[0], after % blocks, after // blocks
    )
    to_prev = remote(
        edge.at[0], halo.at[1], hs_sem.at[0], hr_sem.at[1], before % blocks, before // blocks
    )
    to_next.start()
    to_prev.start()

    strip = min(64, rows)

    def convolve(strips):
        def column(c, carry):
            cols = pl.ds(pl.multiple_of(c * 128, 128), 128)
            for r in strips:
                acc = jnp.zeros((strip, 128), jnp.float32)
                for t in range(taps):
                    e = rim + r + t - half
                    x = extended[e:e + strip, cols] * masks[t, r:r + strip, :]
                    acc = acc + x * depth_ref[t:t + 1, cols]
                mixed[r:r + strip, cols] = acc
            return carry

        lax.fori_loop(0, width // 128, column, 0)

    every = list(range(0, rows, strip))
    convolve(every[1:-1])
    to_next.wait_recv()
    to_prev.wait_recv()
    extended[:rim, :] = halo[0].astype(jnp.float32)
    extended[rim + rows:, :] = halo[1].astype(jnp.float32)
    convolve([every[0], every[-1]])
    normed = normalize(mixed[...], depth_gain_ref[...])
    activated = (normed * jax.nn.sigmoid(normed)).astype(jnp.bfloat16)
    loads[2].wait()
    out_ref[0] = (
        residual[...].astype(jnp.float32)
        + jnp.dot(activated, w_proj[...], preferred_element_type=jnp.float32)
    ).astype(out_ref.dtype)

    for i in range(blocks):
        @pl.when(jnp.logical_not(jnp.logical_and(home, b == i)))
        def _():
            send(i).wait_send()

    to_next.wait_send()
    to_prev.wait_send()


def body(
    frames, utt_lengths, attn_gain, w_qkv, w_out, conv_gain, w_glu, w_depth, depth_gain, w_proj
):
    rows, width = frames.shape[1:]
    blocks, groups = lax.axis_size("blk"), lax.axis_size("grp")
    mixed = projected_and_attended(
        frames[0], utt_lengths, attn_gain, w_qkv, blocks, groups, width // HEADS
    )
    taps = w_depth.shape[0]
    rim = -(-(taps // 2) // 16) * 16
    vm = pl.BlockSpec(memory_space=pltpu.VMEM)
    hbm = pl.BlockSpec(memory_space=pl.ANY)
    return pl.pallas_call(
        functools.partial(finish_kernel, blocks, groups),
        out_shape=jax.ShapeDtypeStruct((1, rows, width), jnp.bfloat16),
        in_specs=[pl.BlockSpec(memory_space=pltpu.SMEM)] + [vm] * 5 + [hbm] * 3,
        out_specs=vm,
        scratch_shapes=[
            pltpu.VMEM((blocks, rows, mixed.shape[1]), jnp.bfloat16),
            pltpu.VMEM(w_out.shape, jnp.bfloat16),
            pltpu.VMEM(w_glu.shape, jnp.bfloat16),
            pltpu.VMEM(w_proj.shape, jnp.bfloat16),
            pltpu.VMEM((taps, rows, 128), jnp.float32),
            pltpu.VMEM((rows, width), jnp.bfloat16),
            pltpu.VMEM((2, rim, width), jnp.bfloat16),
            pltpu.VMEM((2, rim, width), jnp.bfloat16),
            pltpu.VMEM((rows + 2 * rim, width), jnp.float32),
            pltpu.VMEM((rows, width), jnp.float32),
            pltpu.SemaphoreType.DMA((blocks,)),
            pltpu.SemaphoreType.DMA((blocks,)),
            pltpu.SemaphoreType.DMA(()),
            pltpu.SemaphoreType.DMA((3,)),
            pltpu.SemaphoreType.DMA((2,)),
            pltpu.SemaphoreType.DMA((2,)),
        ],
        compiler_params=pltpu.CompilerParams(has_side_effects=True, vmem_limit_bytes=VMEM_LIMIT),
        name="finish",
    )(utt_lengths, mixed, frames[0], conv_gain[None], w_depth, depth_gain[None], w_out, w_glu, w_proj)


def solution(mesh):
    in_specs = (P("grp", "blk", None), P(), P(), P(None, "grp"), P(), P(), P(), P(), P(), P())
    out_specs = P("grp", "blk", None)
    return jax.shard_map(body, mesh=mesh, in_specs=in_specs, out_specs=out_specs, check_vma=False)
```

```python
import functools
import math

import jax
import jax.numpy as jnp
from jax import lax
from jax.experimental import pallas as pl
from jax.experimental.pallas import tpu as pltpu
from jax.sharding import PartitionSpec as P

HEADS = 16

epsilon = 1e-05
big_negative = -1e30
MESH = pl.DeviceIdType.MESH
VMEM_LIMIT = 56 * 1024 * 1024


def normalize(values, row_gain):
    center = values - jnp.mean(values, axis=-1, keepdims=True)
    spread = jnp.mean(center * center, axis=-1, keepdims=True)
    return center * lax.rsqrt(spread + epsilon) * row_gain


def starts_of(lengths_ref):
    starts, total = [], jnp.int32(0)
    for c in range(lengths_ref.shape[0]):
        starts.append(total)
        total = total + lengths_ref[c]
    return starts


def seg_at(starts, positions):
    seg = jnp.full(positions.shape, -1, jnp.int32)
    for start in starts:
        seg = seg + jnp.where(positions >= start, 1, 0)
    return seg


def remote(src, dst, send, recv, blk, grp):
    return pltpu.make_async_remote_copy(
        src_ref=src, dst_ref=dst, send_sem=send, recv_sem=recv,
        device_id=(blk, grp), device_id_type=MESH,
    )


def place_of(window, groups):
    return (window % 2) * (groups // 2) + window // 2


def window_at(place, groups):
    return (place % (groups // 2)) * 2 + place // (groups // 2)


def project_kernel(
    blocks, groups, chunks, head_width, lengths_ref, frames_ref, gain_ref, w_ref,
    q_ref, k_ref, v_ref,
    norm, held, weights, w_sem, d_sem, x_sem, y_sem, p_sem, r_sem,
):
    b, g = lax.axis_index("blk"), lax.axis_index("grp")
    np_ = blocks // groups
    pairs = groups // 2
    rows, width = norm.shape[1:]
    columns = weights.shape[1]
    heads = columns // (3 * head_width)
    place, share, core, chip = b // np_, b % np_, g % 2, g // 2
    mine = window_at(place, groups)
    source_chip = mine // 2
    partner = g + 1 - 2 * core
    if np_ == 1:
        w_src = w_ref
    else:
        w_src = w_ref.at[:, pl.ds(pl.multiple_of(share * columns, 128), columns)]
    w_copy = pltpu.make_async_copy(w_src, weights, w_sem)
    w_copy.start()
    target = place_of(g, groups) * np_ + share
    target_core = place % 2
    self_kept = jnp.logical_and(target == b, target_core == core)

    def direct(c):
        u = b * chunks + c
        return remote(
            norm.at[c], held.at[u], d_sem.at[c], r_sem.at[u], target, 2 * chip + target_core
        )

    for c in range(chunks):
        part = frames_ref[c * rows:(c + 1) * rows, :].astype(jnp.float32)
        norm[c] = normalize(part, gain_ref[...]).astype(jnp.bfloat16)

        @pl.when(jnp.logical_not(self_kept))
        def _():
            direct(c).start()

        @pl.when(self_kept)
        def _():
            held[b * chunks + c] = norm[c]

    lane = lax.broadcasted_iota(jnp.int32, (rows, 128), 1)
    row = lax.broadcasted_iota(jnp.int32, (rows, 128), 0)
    scale = head_width ** (-0.5) * math.log2(math.e)
    starts = starts_of(lengths_ref)

    def padded(part):
        return jnp.concatenate([part, jnp.zeros((rows, 128 - head_width), jnp.float32)], axis=1)

    def project(u):
        out = jnp.dot(held[u], weights[...], preferred_element_type=jnp.float32)
        seg = seg_at(starts, mine * blocks * chunks * rows + u * rows + row)
        same = lane - head_width == seg
        at = pl.ds(pl.multiple_of(u * rows, rows), rows)
        for h in range(heads):
            o = 3 * head_width * h
            q = padded(out[:, o:o + head_width] * scale)
            k = padded(out[:, o + head_width:o + 2 * head_width])
            v = padded(out[:, o + 2 * head_width:o + 3 * head_width])
            q = jnp.where(lane < head_width, q, jnp.where(same, big_negative, 0.0))
            k = jnp.where(lane < head_width, k, jnp.where(same, 0.0, 1.0))
            v = jnp.where(lane < head_width, v, jnp.where(lane == head_width, 1.0, 0.0))
            q_ref[h, at, :] = q.astype(jnp.bfloat16)
            k_ref[h, at, :] = k.astype(jnp.bfloat16)
            v_ref[h, at, :] = v.astype(jnp.bfloat16)

    def pair(u):
        return remote(held.at[u], held.at[u], p_sem.at[u], r_sem.at[u], b, partner)

    def across(u, i):
        other = b - share + (share + i) % np_
        return remote(held.at[u], held.at[u], y_sem.at[u, i], r_sem.at[u], other, g)

    def over(u, k):
        return remote(held.at[u], held.at[u], x_sem.at[u, k], r_sem.at[u], b, 2 * k + core)

    def unit(j, i):
        n = j // chunks
        n = n + place // pairs * (pairs - 1 - 2 * n)
        return ((2 * n + core) * np_ + (share + i) % np_) * chunks + j % chunks

    count = pairs * chunks

    def take(j, carry):
        u = unit(j, 0)

        @pl.when(jnp.logical_not(jnp.logical_and(u // chunks == b, mine == g)))
        def _():
            pair(u).wait_recv()

        for k in range(pairs):
            @pl.when(jnp.logical_and(chip == source_chip, chip != k))
            def _():
                over(u, k).start()

        for i in range(1, np_):
            across(u, i).start()
        pair(u).start()
        return carry

    lax.fori_loop(0, count, take, 0)
    w_copy.wait()

    def own(j, carry):
        project(unit(j, 0))
        return carry

    lax.fori_loop(0, count, own, 0)

    def pass_on(j, carry):
        for i in range(1, np_):
            u = unit(j, i)
            pair(u).wait_recv()
            pair(u).start()
            project(u)
        return carry

    if np_ > 1:
        lax.fori_loop(0, count, pass_on, 0)

    def rest(j, carry):
        n = j // (np_ * chunks)
        n = n + place // pairs * (pairs - 1 - 2 * n)
        i = j // chunks % np_
        u = ((2 * n + 1 - core) * np_ + (share + i) % np_) * chunks + j % chunks
        pair(u).wait_recv()
        project(u)
        return carry

    lax.fori_loop(0, count * np_, rest, 0)

    for c in range(chunks):
        @pl.when(jnp.logical_not(self_kept))
        def _():
            direct(c).wait_send()

    def drain(j, carry):
        u = unit(j, 0)
        for k in range(pairs):
            @pl.when(jnp.logical_and(chip == source_chip, chip != k))
            def _():
                over(u, k).wait_send()

        for i in range(1, np_):
            across(u, i).wait_send()
        for i in range(np_):
            pair(unit(j, i)).wait_send()
        return carry

    lax.fori_loop(0, count, drain, 0)


def attend(head_width, q_ref, k_ref, v_ref, at):
    outs = []
    for h in range(q_ref.shape[0]):
        scores = lax.dot_general(
            q_ref[h, at, :], k_ref[h], (((1,), (1,)), ((), ())),
            preferred_element_type=jnp.float32,
        )
        top = jnp.max(scores, axis=1, keepdims=True)
        weights = jnp.exp2(scores - top).astype(jnp.bfloat16)
        mixed = jnp.dot(weights, v_ref[h], preferred_element_type=jnp.float32)
        outs.append(mixed[:, :head_width] / mixed[:, head_width:head_width + 1])
    return jnp.concatenate(outs, axis=1).astype(jnp.bfloat16)


def projected(frames, lengths, attn_gain, w_qkv, blocks, groups, head_width):
    rows, width = frames.shape
    np_ = blocks // groups
    columns = w_qkv.shape[1] // np_
    heads = columns // (3 * head_width)
    window = rows * blocks
    chunks = 2 if rows % 32 == 0 else 1
    vm = pl.BlockSpec(memory_space=pltpu.VMEM)
    wide = jax.ShapeDtypeStruct((heads, window, 128), jnp.bfloat16)
    return pl.pallas_call(
        functools.partial(project_kernel, blocks, groups, chunks, head_width),
        out_shape=[wide] * 3,
        in_specs=[pl.BlockSpec(memory_space=pltpu.SMEM), vm, vm, pl.BlockSpec(memory_space=pl.ANY)],
        out_specs=[vm] * 3,
        scratch_shapes=[
            pltpu.VMEM((chunks, rows // chunks, width), jnp.bfloat16),
            pltpu.VMEM((blocks * chunks, rows // chunks, width), jnp.bfloat16),
            pltpu.VMEM((width, columns), jnp.bfloat16),
            pltpu.SemaphoreType.DMA(()),
            pltpu.SemaphoreType.DMA((chunks,)),
            pltpu.SemaphoreType.DMA((blocks * chunks, groups // 2)),
            pltpu.SemaphoreType.DMA((blocks * chunks, np_)),
            pltpu.SemaphoreType.DMA((blocks * chunks,)),
            pltpu.SemaphoreType.DMA((blocks * chunks,)),
        ],
        compiler_params=pltpu.CompilerParams(has_side_effects=True, vmem_limit_bytes=VMEM_LIMIT),
        name="project",
    )(lengths, frames, attn_gain[None], w_qkv)


def finish_kernel(
    blocks, groups, head_width, lengths_ref, q_ref, k_ref, v_ref, frames_ref, conv_gain_ref, depth_ref, depth_gain_ref,
    w_out_ref, w_glu_ref, w_proj_ref,
    out_ref,
    mixed_heads, parts, w_out, w_glu, w_proj, masks, residual, edge, halo, extended, mixed,
    s_sem, r_sem, w_sem, hs_sem, hr_sem,
):
    b, g = lax.axis_index("blk"), lax.axis_index("grp")
    np_ = blocks // groups
    rows, width = frames_ref.shape
    taps = depth_ref.shape[0]
    half = (taps - 1) // 2
    rim = halo.shape[1]
    mine, unit = window_at(b // np_, groups), g * np_ + b % np_
    home = mine == g
    position = g * blocks + b
    after = (position + 1) % (blocks * groups)
    before = (position + blocks * groups - 1) % (blocks * groups)

    def send(s):
        return remote(
            mixed_heads.at[s], parts.at[unit], s_sem.at[s], r_sem.at[unit], s, mine
        )

    loads = [
        pltpu.make_async_copy(w_out_ref, w_out, w_sem.at[0]),
        pltpu.make_async_copy(w_glu_ref, w_glu, w_sem.at[1]),
        pltpu.make_async_copy(w_proj_ref, w_proj, w_sem.at[2]),
    ]
    for load in loads:
        load.start()

    def attend_for(i, carry):
        s = (b + 1 + i) % blocks
        at = pl.ds(pl.multiple_of(s * rows, rows), rows)
        mixed_heads[s] = attend(head_width, q_ref, k_ref, v_ref, at)
        kept = jnp.logical_and(home, s == b)

        @pl.when(jnp.logical_not(kept))
        def _():
            send(s).start()

        @pl.when(kept)
        def _():
            parts[unit] = mixed_heads[s]

        return carry

    lax.fori_loop(0, blocks, attend_for, 0)

    row = position * rows + lax.broadcasted_iota(jnp.int32, (rows, 128), 0)
    low = jnp.zeros((rows, 128), jnp.int32)
    high = jnp.full((rows, 128), blocks * groups * rows, jnp.int32)
    for start in starts_of(lengths_ref):
        low = jnp.where(row >= start, jnp.maximum(low, start), low)
        high = jnp.where(row < start, jnp.minimum(high, start), high)
    for t in range(taps):
        at = row + (t - half)
        masks[t] = jnp.where(jnp.logical_and(at >= low, at < high), 1.0, 0.0)

    for i in range(blocks):
        @pl.when(jnp.logical_not(jnp.logical_and(home, unit == i)))
        def _():
            remote(parts.at[i], parts.at[i], s_sem.at[i], r_sem.at[i], b, g).wait_recv()

    attended = jnp.concatenate([parts[i] for i in range(blocks)], axis=1)
    loads[0].wait()
    total = frames_ref[...].astype(jnp.float32) + jnp.dot(
        attended, w_out[...], preferred_element_type=jnp.float32
    )
    residual[...] = total.astype(jnp.bfloat16)
    conv_in = normalize(residual[...].astype(jnp.float32), conv_gain_ref[...]).astype(jnp.bfloat16)
    loads[1].wait()
    step = 256
    for n in range(0, width, step):
        a = jnp.dot(conv_in, w_glu[:, n:n + step], preferred_element_type=jnp.float32)
        gate = jnp.dot(
            conv_in, w_glu[:, width + n:width + n + step], preferred_element_type=jnp.float32
        )
        gated = (a * jax.nn.sigmoid(gate)).astype(jnp.bfloat16)
        edge[0, :, n:n + step] = gated[:rim]
        edge[1, :, n:n + step] = gated[rows - rim:]
        extended[rim:rim + rows, n:n + step] = gated.astype(jnp.float32)

    to_next = remote(
        edge.at[1], halo.at[0], hs_sem.at[1], hr_sem.at[0], after % blocks, after // blocks
    )
    to_prev = remote(
        edge.at[0], halo.at[1], hs_sem.at[0], hr_sem.at[1], before % blocks, before // blocks
    )
    to_next.start()
    to_prev.start()

    strip = min(64, rows)

    def convolve(strips):
        def column(c, carry):
            cols = pl.ds(pl.multiple_of(c * 128, 128), 128)
            for r in strips:
                acc = jnp.zeros((strip, 128), jnp.float32)
                for t in range(taps):
                    e = rim + r + t - half
                    x = extended[e:e + strip, cols] * masks[t, r:r + strip, :]
                    acc = acc + x * depth_ref[t:t + 1, cols]
                mixed[r:r + strip, cols] = acc
            return carry

        lax.fori_loop(0, width // 128, column, 0)

    every = list(range(0, rows, strip))
    convolve(every[1:-1])
    to_next.wait_recv()
    to_prev.wait_recv()
    extended[:rim, :] = halo[0].astype(jnp.float32)
    extended[rim + rows:, :] = halo[1].astype(jnp.float32)
    convolve([every[0], every[-1]])
    normed = normalize(mixed[...], depth_gain_ref[...])
    activated = (normed * jax.nn.sigmoid(normed)).astype(jnp.bfloat16)
    loads[2].wait()
    out_ref[0] = (
        residual[...].astype(jnp.float32)
        + jnp.dot(activated, w_proj[...], preferred_element_type=jnp.float32)
    ).astype(out_ref.dtype)

    for i in range(blocks):
        @pl.when(jnp.logical_not(jnp.logical_and(home, b == i)))
        def _():
            send(i).wait_send()

    to_next.wait_send()
    to_prev.wait_send()


def body(
    frames, utt_lengths, attn_gain, w_qkv, w_out, conv_gain, w_glu, w_depth, depth_gain, w_proj
):
    rows, width = frames.shape[1:]
    blocks, groups = lax.axis_size("blk"), lax.axis_size("grp")
    head_width = width // HEADS
    q, k, v = projected(frames[0], utt_lengths, attn_gain, w_qkv, blocks, groups, head_width)
    taps = w_depth.shape[0]
    rim = -(-(taps // 2) // 16) * 16
    vm = pl.BlockSpec(memory_space=pltpu.VMEM)
    hbm = pl.BlockSpec(memory_space=pl.ANY)
    return pl.pallas_call(
        functools.partial(finish_kernel, blocks, groups, head_width),
        out_shape=jax.ShapeDtypeStruct((1, rows, width), jnp.bfloat16),
        in_specs=[pl.BlockSpec(memory_space=pltpu.SMEM)] + [vm] * 7 + [hbm] * 3,
        out_specs=vm,
        scratch_shapes=[
            pltpu.VMEM((blocks, rows, q.shape[0] * head_width), jnp.bfloat16),
            pltpu.VMEM((blocks, rows, q.shape[0] * head_width), jnp.bfloat16),
            pltpu.VMEM(w_out.shape, jnp.bfloat16),
            pltpu.VMEM(w_glu.shape, jnp.bfloat16),
            pltpu.VMEM(w_proj.shape, jnp.bfloat16),
            pltpu.VMEM((taps, rows, 128), jnp.float32),
            pltpu.VMEM((rows, width), jnp.bfloat16),
            pltpu.VMEM((2, rim, width), jnp.bfloat16),
            pltpu.VMEM((2, rim, width), jnp.bfloat16),
            pltpu.VMEM((rows + 2 * rim, width), jnp.float32),
            pltpu.VMEM((rows, width), jnp.float32),
            pltpu.SemaphoreType.DMA((blocks,)),
            pltpu.SemaphoreType.DMA((blocks,)),
            pltpu.SemaphoreType.DMA((3,)),
            pltpu.SemaphoreType.DMA((2,)),
            pltpu.SemaphoreType.DMA((2,)),
        ],
        compiler_params=pltpu.CompilerParams(has_side_effects=True, vmem_limit_bytes=VMEM_LIMIT),
        name="finish",
    )(
        utt_lengths, q, k, v, frames[0], conv_gain[None], w_depth, depth_gain[None],
        w_out, w_glu, w_proj,
    )


def solution(mesh):
    in_specs = (P("grp", "blk", None), P(), P(), P(None, "grp"), P(), P(), P(), P(), P(), P())
    out_specs = P("grp", "blk", None)
    return jax.shard_map(body, mesh=mesh, in_specs=in_specs, out_specs=out_specs, check_vma=False)
```
